32 devices in a mesh: hist: 16 (over z, x, core), orb: 2 (over y).
Axes of the slice: x: 2, y: 2, z: 4, core: 2. Of those that a mesh axis runs over, the one named last changes fastest.
Arguments:
- g_hist: bfloat16 [32, 64, 2048], P('hist', 'orb'), may hold values from -6 to 6
- sigma_hist: bfloat16 [2, 64, 2048], P(None, None, 'hist'), may hold values from -0.125 to 0.125
- diag_inv: float32 [32, 64, 64], P('hist'), may hold values from -0.75 to 0.75
- previous: float32 [2, 32, 64, 64], P(None, 'hist', 'orb'), may hold values from -6 to 6
- block_of_slot: int32 [16], replicated, may hold values from 0 to 15, each once
- front_pos: int32 [2], replicated, may hold values from 16 to 31
Outputs:
- g_row: float32 [2, 32, 64, 64], P(None, 'hist', 'orb')
- sigma_row: float32 [2, 32, 64, 64], P(None, 'hist', 'orb')
The draws below stay inside these ranges and needn't reach their ends.
Inputs may be any that keep to these rules, and one draw needn't show every extreme that they name: `block_of_slot`: every block index appears once.
All inputs are finite; a program needn't handle non-finite values.
Results may differ from the reference program's by a relative error of at most 0.0003.
Values may be sent and summed in bfloat16 or wider, within the bound.
A program may use at most 64 MiB of HBM per device.

```python
import jax
import jax.numpy as jnp
from jax import lax

O = 64
TB = 2
NT = 32
N_HIST = 16


def shard_levels(own_key, dims, split, low, largest):
    level = 1.0
    for axis_at, blocks in split:
        steps = jax.random.uniform(jax.random.fold_in(jax.random.fold_in(own_key, 6), axis_at), (blocks,), jnp.float32, low / len(split), largest / len(split))
        level = level * jnp.repeat(jnp.exp(steps), dims[axis_at] // blocks).reshape((-1,) + (1,) * (len(dims) - 1 - axis_at))
    return level


def noise(own_key, dims, spread, bound, shards=(), held_as=jnp.bfloat16):
    gain = shard_levels(own_key, dims, shards, -0.22, 0.18) if shards else 1.0
    values = jax.random.normal(own_key, dims, jnp.float32) * spread * gain
    return jnp.minimum(jnp.maximum(values, -bound), bound).astype(held_as)


def setup_inputs(seed: int = 0) -> dict:
    key_list = jax.random.split(jax.random.key(seed), 7)
    return {
        "g_hist": noise(key_list[0], (NT, O, NT * O), 1.0, 6.0, ((0, 16), (1, 2))),
        "sigma_hist": noise(key_list[1], (2, O, NT * O), (NT * O) ** -0.5, 0.125, ((2, 16),)),
        "diag_inv": noise(key_list[2], (NT, O, O), O ** -0.5, 0.75, ((0, 16),), jnp.float32),
        "previous": noise(key_list[3], (2, NT, O, O), 1.0, 6.0, ((1, 16), (2, 2)), jnp.float32),
        "block_of_slot": jax.random.permutation(key_list[4], N_HIST).astype(jnp.int32),
        "front_pos": jax.random.randint(key_list[5], (2,), NT // 2, NT).astype(jnp.int32),
    }


COUPLING = 0.5


def reference(g_hist, sigma_hist, diag_inv, previous, block_of_slot, front_pos):
    slot_rows = jnp.arange(NT, dtype=jnp.int32)
    col_time = (block_of_slot[slot_rows // TB] * TB + slot_rows % TB).astype(jnp.int32)
    times = (jnp.arange(NT * O, dtype=jnp.int32) // O).astype(jnp.int32)
    front_keep = times[None, :] <= front_pos[:, None]
    sigma_kept = jnp.where(front_keep[:, None, :], sigma_hist, jnp.zeros_like(sigma_hist)).astype(jnp.float32)

    def column(item):
        g_one, when = item
        g_kept = jnp.where((times >= when)[None, :], g_one, jnp.zeros_like(g_one)).astype(jnp.float32)
        return jnp.einsum("cx,fax->fca", g_kept, sigma_kept)

    integral = lax.map(column, (g_hist, col_time))
    integral = jnp.transpose(integral, (1, 0, 2, 3))
    combined = previous + integral
    rows = diag_inv[front_pos]
    g_row = jnp.einsum("ftcb,fab->ftca", combined, rows, precision=lax.Precision.HIGHEST)
    sigma_row = COUPLING * g_row * g_row * jnp.swapaxes(g_row, 2, 3)
    return g_row, sigma_row
```

```python
import functools

import jax
import jax.numpy as jnp
from jax import lax
from jax.experimental import pallas as pl
from jax.experimental.pallas import tpu as pltpu
from jax.sharding import PartitionSpec as P

COUPLING = 0.5
MESH = pl.DeviceIdType.MESH


def xor(a, b, size):
    out, bit = 0, 1
    while bit < size:
        out = out + bit * ((a // bit + b // bit) % 2)
        bit *= 2
    return out


def loop(low, high, step):
    if high - low <= 8:
        for i in range(low, high):
            step(i)
    else:
        lax.fori_loop(low, high, lambda i, c: (step(i), c)[1], 0)


def kernel(lines, blocks_ref, front_ref, g_hbm, s_hbm, d_hbm, p_hbm, g_out, s_out,
           g_v, all_s, d_v, p_v, acc, d_mine, d_core, d_x, d_z, d_part, d_all,
           t_send, t_recv, loc_sem, z_send, z_recv, x_send, x_recv, c_send, c_recv,
           d_send, d_recv, t_sems):
    cols, half = g_hbm.shape[0], g_hbm.shape[1]
    orb, lanes = s_hbm.shape[1], s_hbm.shape[2]
    me = lax.axis_index("hist")
    o = lax.axis_index("orb")
    core = me % 2
    xi = (me // 2) % 2
    z = me // 4
    quarter = orb // 4

    def at(zz, xx, cc):
        return (zz * 2 + xx) * 2 + cc

    core_peer = (at(z, xi, 1 - core), o)
    x_peer = (at(z, 1 - xi, core), o)
    y_peer = (me, 1 - o)
    yc_peer = (at(z, xi, 1 - core), 1 - o)

    def z_peer(d):
        return (at(xor(z, d, lines), xi, core), o)

    load_s = pltpu.make_async_copy(s_hbm, all_s.at[z, xi, core], loc_sem.at[0])
    load_d = pltpu.make_async_copy(d_hbm, d_v, loc_sem.at[1])
    load_g = pltpu.make_async_copy(g_hbm, g_v, loc_sem.at[2])
    load_p = pltpu.make_async_copy(p_hbm, p_v, loc_sem.at[3])
    load_s.start()
    load_d.start()
    load_g.start()
    load_p.start()

    barrier = pltpu.get_barrier_semaphore()

    def greet(peer):
        pl.semaphore_signal(barrier, inc=1, device_id=peer, device_id_type=MESH)

    loop(1, lines, lambda d: greet(z_peer(d)))
    for peer in (x_peer, core_peer, y_peer, yc_peer):
        greet(peer)
    pl.semaphore_wait(barrier, lines + 3)

    def send(src, dst, ssem, rsem, peer):
        return pltpu.make_async_remote_copy(
            src_ref=src, dst_ref=dst, send_sem=ssem, recv_sem=rsem,
            device_id=peer, device_id_type=MESH)

    def piece(d, xx, cc):
        return all_s.at[xor(z, d, lines), xx, cc]

    def z_copy(d):
        return send(piece(0, xi, core), piece(0, xi, core), z_send.at[d], z_recv.at[d], z_peer(d))

    def x_copy(d):
        return send(piece(d, xi, core), piece(d, xi, core), x_send.at[d], x_recv.at[d], x_peer)

    def c_copy(d, other):
        xx = xi + other - 2 * xi * other
        k = other * lines + d
        return send(piece(d, xx, core), piece(d, xx, core), c_send.at[k], c_recv.at[k], core_peer)

    load_s.wait()
    loop(1, lines, lambda d: z_copy(lines - d).start())
    x_copy(0).start()
    c_copy(0, 0).start()

    load_d.wait()

    def rows_of(q):
        part = []
        for f in range(2):
            when = front_ref[f]
            mine = (when // cols) == me
            got = d_v[when % cols, pl.ds(pl.multiple_of(q * quarter, 8), quarter), :]
            part.append(jnp.where(mine, got, jnp.zeros_like(got)))
        return jnp.concatenate(part, axis=1)

    my_q = o * 2 + core
    d_mine[...] = rows_of(o * 2 + 1 - core)
    d_c = send(d_mine, d_core, d_send.at[0], d_recv.at[0], core_peer)
    d_c.start()
    own_rows = rows_of(my_q)
    load_g.wait()
    acc[...] = jnp.zeros_like(acc)

    col0 = blocks_ref[me] * cols

    def product(d, xx):
        chip = xor(z, d, lines) * 2 + xx
        width = 2 * lanes
        start = pl.multiple_of(chip * width, width)
        time = (lax.broadcasted_iota(jnp.int32, (1, width), 1) + start) // orb
        one, zero = jnp.float32(1), jnp.float32(0)
        left = jnp.concatenate(
            [g_v[t, :, pl.ds(start, width)]
             * jnp.where(time >= col0 + t, one, zero).astype(jnp.bfloat16)
             for t in range(cols)], axis=0)
        zz = xor(z, d, lines)
        both = jnp.concatenate([all_s[zz, xx, 0], all_s[zz, xx, 1]], axis=2)
        right = jnp.concatenate(
            [both[f] * jnp.where(time <= front_ref[f], one, zero).astype(jnp.bfloat16)
             for f in range(2)], axis=0)
        acc[...] += lax.dot_general(left, right, (((1,), (1,)), ((), ())),
                                    preferred_element_type=jnp.float32)

    d_c.wait()
    d_x[0] = own_rows + d_core[...]
    d_xc = send(d_x.at[0], d_x.at[1], d_send.at[1], d_recv.at[1], x_peer)
    d_xc.start()

    def relay(d):
        z_copy(d).wait_recv()
        x_copy(d).start()
        c_copy(d, 0).start()

    relay(1)
    d_xc.wait()
    d_z[0] = d_x[0] + d_x[1]

    def dz_copy(d):
        return send(d_z.at[0], d_z.at[d], d_send.at[5 + d], d_recv.at[5 + d], z_peer(d))

    loop(1, lines, lambda d: dz_copy(d).start())
    loop(2, lines, relay)

    c_copy(0, 0).wait_recv()
    product(0, xi)

    def relay_x(d):
        x_copy(d).wait_recv()
        c_copy(d, 1).start()

    def near(d):
        relay_x(d - 1)
        c_copy(d, 0).wait_recv()
        product(d, xi)

    loop(1, lines, near)

    loop(1, lines, lambda d: dz_copy(d).wait())
    total = d_z[0]
    total = lax.fori_loop(1, lines, lambda d, t: t + d_z[d], total)
    d_part[...] = total
    outs = [send(d_part, d_all.at[my_q], d_send.at[2 + k], d_recv.at[2 + k], peer)
            for k, peer in enumerate((core_peer, y_peer, yc_peer))]
    for c in outs:
        c.start()
    d_all[my_q] = total
    relay_x(lines - 1)

    def far(d):
        c_copy(d, 1).wait_recv()
        product(d, 1 - xi)

    loop(0, lines, far)

    load_p.wait()
    prev = jnp.concatenate([p_v[f].reshape(cols * half, orb) for f in range(2)], axis=1)
    combined = acc[...] + prev
    for c in outs:
        c.wait()
    rows = d_all[...].reshape(orb, 2 * orb)
    lane = lax.broadcasted_iota(jnp.int32, rows.shape, 1)
    none = jnp.zeros_like(rows)
    weight = jnp.concatenate(
        [jnp.where(lane < orb, rows, none), jnp.where(lane < orb, none, rows)], axis=0)
    contract = (((1,), (1,)), ((), ()))
    flipped = lax.dot_general(weight, combined, contract, precision=lax.Precision.HIGHEST,
                              preferred_element_type=jnp.float32)

    def block(which):
        parts = []
        for f in range(2):
            low = flipped[f * orb:f * orb + half]
            high = flipped[f * orb + half:f * orb + 2 * half]
            parts.append(jnp.where(which == 0, low, high))
        return jnp.concatenate(parts, axis=1)

    t_send[...] = block(1 - o)
    t_copy = send(t_send, t_recv, t_sems.at[0], t_sems.at[1], y_peer)
    t_copy.start()
    g_new = lax.dot_general(combined, weight, contract, precision=lax.Precision.HIGHEST,
                            preferred_element_type=jnp.float32)
    scaled = COUPLING * g_new * g_new
    own = block(o)
    for f in range(2):
        for t in range(cols):
            g_out[f, t] = g_new[t * half:(t + 1) * half, f * orb:(f + 1) * orb]
    t_copy.wait()
    other = t_recv[...]
    first = jnp.where(o == 0, own, other)
    second = jnp.where(o == 0, other, own)
    for f in range(2):
        for t in range(cols):
            k = (f * cols + t) * half
            mirror = jnp.concatenate([first[:, k:k + half], second[:, k:k + half]], axis=1)
            s_out[f, t] = scaled[t * half:(t + 1) * half, f * orb:(f + 1) * orb] * mirror

    loop(1, lines, lambda d: z_copy(d).wait_send())
    loop(0, lines, lambda d: x_copy(d).wait_send())
    loop(0, lines, lambda d: c_copy(d, 0).wait_send())
    loop(0, lines, lambda d: c_copy(d, 1).wait_send())


def body(lines, g_hist, sigma_hist, diag_inv, previous, block_of_slot, front_pos):
    cols, half, depth = g_hist.shape
    orb, lanes = sigma_hist.shape[1], sigma_hist.shape[2]
    quarter = orb // 4
    out = jax.ShapeDtypeStruct(previous.shape, jnp.float32)
    smem = pl.BlockSpec(memory_space=pltpu.SMEM)
    hbm = pl.BlockSpec(memory_space=pl.ANY)
    vmem = pl.BlockSpec(memory_space=pltpu.VMEM)
    dma = pltpu.SemaphoreType.DMA
    f32 = jnp.float32
    flops = 2 * cols * half * depth * 2 * orb
    return pl.pallas_call(
        functools.partial(kernel, lines),
        out_shape=(out, out),
        in_specs=[smem, smem, hbm, hbm, hbm, hbm],
        out_specs=(vmem, vmem),
        scratch_shapes=[
            pltpu.VMEM(g_hist.shape, g_hist.dtype),
            pltpu.VMEM((lines, 2, 2) + sigma_hist.shape, sigma_hist.dtype),
            pltpu.VMEM(diag_inv.shape, f32),
            pltpu.VMEM(previous.shape, f32),
            pltpu.VMEM((cols * half, 2 * orb), f32),
            pltpu.VMEM((quarter, 2 * orb), f32),
            pltpu.VMEM((quarter, 2 * orb), f32),
            pltpu.VMEM((2, quarter, 2 * orb), f32),
            pltpu.VMEM((lines, quarter, 2 * orb), f32),
            pltpu.VMEM((quarter, 2 * orb), f32),
            pltpu.VMEM((4, quarter, 2 * orb), f32),
            pltpu.VMEM((half, 2 * cols * half), f32),
            pltpu.VMEM((half, 2 * cols * half), f32),
            dma((4,)),
            dma((lines,)), dma((lines,)),
            dma((lines,)), dma((lines,)),
            dma((2 * lines,)), dma((2 * lines,)),
            dma((5 + lines,)), dma((5 + lines,)),
            dma((2,)),
        ],
        compiler_params=pltpu.CompilerParams(collective_id=0, has_side_effects=True),
        cost_estimate=pl.CostEstimate(flops=flops, bytes_accessed=2 * g_hist.size, transcendentals=0),
    )(block_of_slot, front_pos, g_hist, sigma_hist, diag_inv, previous)


def solution(mesh):
    lines = mesh.shape["hist"] // 4
    in_specs = (
        P("hist", "orb", None),
        P(None, None, "hist"),
        P("hist", None, None),
        P(None, "hist", "orb", None),
        P(),
        P(),
    )
    out_specs = (P(None, "hist", "orb", None), P(None, "hist", "orb", None))
    return jax.shard_map(functools.partial(body, lines), mesh=mesh, in_specs=in_specs,
                         out_specs=out_specs, check_vma=False)
```

```python
import functools

import jax
import jax.numpy as jnp
from jax import lax
from jax.experimental import pallas as pl
from jax.experimental.pallas import tpu as pltpu
from jax.sharding import PartitionSpec as P

COUPLING = 0.5
MESH = pl.DeviceIdType.MESH


def xor(a, b, size):
    out, bit = 0, 1
    while bit < size:
        out = out + bit * ((a // bit + b // bit) % 2)
        bit *= 2
    return out


def loop(low, high, step):
    if high - low <= 8:
        for i in range(low, high):
            step(i)
    else:
        lax.fori_loop(low, high, lambda i, c: (step(i), c)[1], 0)


def kernel(lines, blocks_ref, front_ref, g_hbm, s_hbm, d_hbm, p_hbm, out,
           g_v, all_s, d_v, p_v, acc, d_out, d_in, d_z, d_all, packed,
           loc_sem, z_send, z_recv, x_send, x_recv, c_send, c_recv,
           d_send, d_recv, dz_send, dz_recv, y_send, y_recv):
    cols, half = g_hbm.shape[0], g_hbm.shape[1]
    orb, lanes = s_hbm.shape[1], s_hbm.shape[2]
    me = lax.axis_index("hist")
    o = lax.axis_index("orb")
    core = me % 2
    xi = (me // 2) % 2
    z = me // 4
    rows = orb // 2

    def at(zz, xx, cc):
        return (zz * 2 + xx) * 2 + cc

    core_peer = (at(z, xi, 1 - core), o)
    x_peer = (at(z, 1 - xi, core), o)
    xc_peer = (at(z, 1 - xi, 1 - core), o)
    y_peer = (me, 1 - o)

    def z_peer(d):
        return (at(xor(z, d, lines), xi, core), o)

    load_s = pltpu.make_async_copy(s_hbm.at[o], all_s.at[z, xi, core], loc_sem.at[0])
    load_d = pltpu.make_async_copy(d_hbm, d_v, loc_sem.at[1])
    load_g = pltpu.make_async_copy(g_hbm, g_v.at[o], loc_sem.at[2])
    load_p = pltpu.make_async_copy(p_hbm.at[o], p_v.at[o], loc_sem.at[3])
    load_s.start()
    load_d.start()
    load_g.start()
    load_p.start()

    barrier = pltpu.get_barrier_semaphore()

    def greet(peer):
        pl.semaphore_signal(barrier, inc=1, device_id=peer, device_id_type=MESH)

    loop(1, lines, lambda d: greet(z_peer(d)))
    for peer in (x_peer, xc_peer, core_peer, y_peer):
        greet(peer)

    def rows_of(part):
        when = front_ref[o]
        mine = (when // cols) == me
        first = pl.multiple_of(part * rows, 8)
        got = d_v[when % cols, pl.ds(first, rows), :]
        wide = jnp.concatenate([got[:rows // 2], got[rows // 2:]], axis=1)
        return jnp.where(mine, wide, jnp.zeros_like(wide))

    load_d.wait()
    d_out[0] = rows_of(core)
    d_out[1] = rows_of(1 - core)
    acc[...] = jnp.zeros_like(acc)
    load_s.wait()
    pl.semaphore_wait(barrier, lines + 3)

    def send(src, dst, ssem, rsem, peer):
        return pltpu.make_async_remote_copy(
            src_ref=src, dst_ref=dst, send_sem=ssem, recv_sem=rsem,
            device_id=peer, device_id_type=MESH)

    def piece(d, xx, cc):
        return all_s.at[xor(z, d, lines), xx, cc]

    def z_copy(d):
        return send(piece(0, xi, core), piece(0, xi, core), z_send.at[d], z_recv.at[d], z_peer(d))

    def x_copy(d):
        return send(piece(d, xi, core), piece(d, xi, core), x_send.at[d], x_recv.at[d], x_peer)

    def c_copy(d, other):
        xx = xi + other - 2 * xi * other
        k = other * lines + d
        return send(piece(d, xx, core), piece(d, xx, core), c_send.at[k], c_recv.at[k], core_peer)

    d_copies = [send(d_out.at[which], d_in.at[k], d_send.at[k], d_recv.at[k], peer)
                for k, (which, peer) in enumerate(((0, x_peer), (1, xc_peer), (1, core_peer)))]
    for c in d_copies:
        c.start()
    x_copy(0).start()
    loop(1, lines, lambda d: z_copy(lines - d).start())
    c_copy(0, 0).start()
    load_g.wait()
    g_copy = send(g_v.at[o], g_v.at[o], y_send.at[0], y_recv.at[0], y_peer)
    p_copy = send(p_hbm.at[1 - o], p_v.at[o], y_send.at[1], y_recv.at[1], y_peer)
    g_copy.start()
    p_copy.start()

    col0 = blocks_ref[me] * cols

    def product(d, xx):
        zz = xor(z, d, lines)
        width = 2 * lanes
        start = pl.multiple_of((zz * 2 + xx) * width, width)
        time = (lax.broadcasted_iota(jnp.int32, (1, width), 1) + start) // orb
        one, zero = jnp.float32(1), jnp.float32(0)
        left = []
        for t in range(cols):
            keep = jnp.where((time >= col0 + t) & (time <= front_ref[o]), one, zero)
            keep = keep.astype(jnp.bfloat16)
            left += [g_v[h, t, :, pl.ds(start, width)] * keep for h in range(2)]
        right = jnp.concatenate([all_s[zz, xx, 0], all_s[zz, xx, 1]], axis=1)
        acc[...] += lax.dot_general(jnp.concatenate(left, axis=0), right, (((1,), (1,)), ((), ())),
                                    preferred_element_type=jnp.float32)

    def relay(d):
        z_copy(d).wait_recv()
        x_copy(d).start()
        c_copy(d, 0).start()

    def relay_x(d):
        x_copy(d).wait_recv()
        c_copy(d, 1).start()

    def near(d):
        c_copy(d, 0).wait_recv()
        product(d, xi)

    def far(d):
        c_copy(d, 1).wait_recv()
        product(d, 1 - xi)

    def dz_copy(d):
        return send(d_z.at[0], d_z.at[d], dz_send.at[d], dz_recv.at[d], z_peer(d))

    relay_x(0)
    for c in d_copies:
        c.wait()
    d_z[0] = (d_out[0] + d_in[0]) + (d_in[1] + d_in[2])
    loop(1, lines, lambda d: dz_copy(d).start())
    loop(1, lines, relay)
    loop(1, lines - 1, relay_x)
    g_copy.wait_recv()
    near(0)
    near(1)
    relay_x(lines - 1)
    loop(1, lines, lambda d: dz_copy(d).wait())
    total = lax.fori_loop(1, lines, lambda d, t: t + d_z[d], d_z[0])
    d_all[core] = total
    d_last = send(d_all.at[core], d_all.at[core], d_send.at[3], d_recv.at[3], core_peer)
    d_last.start()
    loop(2, lines, near)
    loop(0, lines, far)

    load_p.wait()
    p_copy.wait()
    prev = jnp.concatenate([p_v[h, t] for t in range(cols) for h in range(2)], axis=0)
    combined = acc[...] + prev
    d_last.wait()
    weight = jnp.concatenate([d_all[c][:, k * orb:(k + 1) * orb]
                              for c in range(2) for k in range(2)], axis=0)
    contract = (((1,), (1,)), ((), ()))
    high = dict(precision=lax.Precision.HIGHEST, preferred_element_type=jnp.float32)
    flipped = lax.dot_general(weight, combined, contract, **high)
    g_new = lax.dot_general(combined, weight, contract, **high)
    t_copies = []
    for t in range(cols):
        g_t = g_new[t * orb:(t + 1) * orb]
        s_t = COUPLING * g_t * g_t * flipped[:, t * orb:(t + 1) * orb]
        done = jnp.concatenate([g_t, s_t], axis=1)
        packed[t] = jnp.where(o == 0, done[half:], done[:half])
        c = send(packed.at[t], out.at[o, t], y_send.at[2 + t], y_recv.at[2 + t], y_peer)
        c.start()
        t_copies.append(c)
        out[o, t] = jnp.where(o == 0, done[:half], done[half:])

    g_copy.wait_send()
    loop(1, lines, lambda d: z_copy(d).wait_send())
    loop(0, lines, lambda d: x_copy(d).wait_send())
    loop(0, lines, lambda d: c_copy(d, 0).wait_send())
    loop(0, lines, lambda d: c_copy(d, 1).wait_send())
    for c in t_copies:
        c.wait()


def body(lines, g_hist, sigma_hist, diag_inv, previous, block_of_slot, front_pos):
    cols, half, depth = g_hist.shape
    orb, lanes = sigma_hist.shape[1], sigma_hist.shape[2]
    smem = pl.BlockSpec(memory_space=pltpu.SMEM)
    hbm = pl.BlockSpec(memory_space=pl.ANY)
    dma = pltpu.SemaphoreType.DMA
    f32 = jnp.float32
    part = (orb // 4, 2 * orb)
    flops = 2 * cols * orb * depth * orb
    out = pl.pallas_call(
        functools.partial(kernel, lines),
        out_shape=pltpu.VMEM((2, cols, half, 2 * orb), f32),
        in_specs=[smem, smem, hbm, hbm, hbm, hbm],
        out_specs=pl.BlockSpec(memory_space=pltpu.VMEM),
        scratch_shapes=[
            pltpu.VMEM((2,) + g_hist.shape, g_hist.dtype),
            pltpu.VMEM((lines, 2, 2, orb, lanes), sigma_hist.dtype),
            pltpu.VMEM(diag_inv.shape, f32),
            pltpu.VMEM((2,) + previous.shape[1:], f32),
            pltpu.VMEM((cols * orb, orb), f32),
            pltpu.VMEM((2,) + part, f32),
            pltpu.VMEM((3,) + part, f32),
            pltpu.VMEM((lines,) + part, f32),
            pltpu.VMEM((2,) + part, f32),
            pltpu.VMEM((cols, half, 2 * orb), f32),
            dma((4,)),
            dma((lines,)), dma((lines,)),
            dma((lines,)), dma((lines,)),
            dma((2 * lines,)), dma((2 * lines,)),
            dma((4,)), dma((4,)),
            dma((lines,)), dma((lines,)),
            dma((2 + cols,)), dma((2 + cols,)),
        ],
        compiler_params=pltpu.CompilerParams(collective_id=0, has_side_effects=True),
        cost_estimate=pl.CostEstimate(flops=flops, bytes_accessed=2 * g_hist.size, transcendentals=0),
    )(block_of_slot, front_pos, g_hist, sigma_hist, diag_inv, previous)
    return out[..., :orb], out[..., orb:]


def solution(mesh):
    lines = mesh.shape["hist"] // 4
    in_specs = (
        P("hist", "orb", None),
        P(None, None, "hist"),
        P("hist", None, None),
        P(None, "hist", "orb", None),
        P(),
        P(),
    )
    out_specs = (P(None, "hist", "orb", None), P(None, "hist", "orb", None))
    return jax.shard_map(functools.partial(body, lines), mesh=mesh, in_specs=in_specs,
                         out_specs=out_specs, check_vma=False)
```

```python
import functools

import jax
import jax.numpy as jnp
from jax import lax
from jax.experimental import pallas as pl
from jax.experimental.pallas import tpu as pltpu
from jax.sharding import PartitionSpec as P

COUPLING = 0.5
MESH = pl.DeviceIdType.MESH


def loop(low, high, step):
    if high - low <= 8:
        for i in range(low, high):
            step(i)
    else:
        lax.fori_loop(low, high, lambda i, c: (step(i), c)[1], 0)


def kernel(lines, blocks_ref, front_ref, g_hbm, s_hbm, d_hbm, p_hbm, out,
           g_v, all_s, d_v, p_v, acc, d_out, d_in, d_z, d_up, d_all, packed,
           loc_sem, z_send, u_send, z_recv, x_send, x_recv, c_send, c_recv,
           d_send, d_recv, dz_send, dz_recv, du_send, y_send, y_recv):
    cols, half = g_hbm.shape[0], g_hbm.shape[1]
    orb, lanes = s_hbm.shape[1], s_hbm.shape[2]
    me = lax.axis_index("hist")
    o = lax.axis_index("orb")
    core = me % 2
    xi = (me // 2) % 2
    z = me // 4
    rows = orb // 2

    def at(zz, xx, cc):
        return (zz * 2 + xx) * 2 + cc

    core_peer = (at(z, xi, 1 - core), o)
    x_peer = (at(z, 1 - xi, core), o)
    xc_peer = (at(z, 1 - xi, 1 - core), o)
    y_peer = (me, 1 - o)

    def z_peer(zz):
        return (at(zz, xi, core), o)

    not_top = z + 1 < lines

    def source(j):
        return jnp.where(j <= z, z - j, j)

    load_s = pltpu.make_async_copy(s_hbm.at[o], all_s.at[z, xi, core], loc_sem.at[0])
    load_d = pltpu.make_async_copy(d_hbm, d_v, loc_sem.at[1])
    load_g = pltpu.make_async_copy(g_hbm, g_v.at[o], loc_sem.at[2])
    load_p = pltpu.make_async_copy(p_hbm.at[o], p_v.at[o], loc_sem.at[3])
    load_s.start()
    load_d.start()
    load_g.start()
    load_p.start()

    barrier = pltpu.get_barrier_semaphore()

    def greet(peer):
        pl.semaphore_signal(barrier, inc=1, device_id=peer, device_id_type=MESH)

    @pl.when(z > 0)
    def _():
        greet(z_peer(z - 1))

    def greet_above(d):
        @pl.when(z + d < lines)
        def _():
            greet(z_peer(z + d))

    loop(1, lines, greet_above)
    for peer in (x_peer, xc_peer, core_peer, y_peer):
        greet(peer)

    def rows_of(part):
        when = front_ref[o]
        mine = (when // cols) == me
        first = pl.multiple_of(part * rows, 8)
        got = d_v[when % cols, pl.ds(first, rows), :]
        wide = jnp.concatenate([got[:rows // 2], got[rows // 2:]], axis=1)
        return jnp.where(mine, wide, jnp.zeros_like(wide))

    load_d.wait()
    d_out[0] = rows_of(core)
    d_out[1] = rows_of(1 - core)
    acc[...] = jnp.zeros_like(acc)
    load_s.wait()
    pl.semaphore_wait(barrier, 4 + z + jnp.where(not_top, 1, 0))

    def send(src, dst, ssem, rsem, peer):
        return pltpu.make_async_remote_copy(
            src_ref=src, dst_ref=dst, send_sem=ssem, recv_sem=rsem,
            device_id=peer, device_id_type=MESH)

    def down_copy(d):
        ref = all_s.at[z, xi, core]
        return send(ref, ref, z_send.at[d], z_recv.at[z], z_peer(z - d))

    def up_copy(src):
        ref = all_s.at[src, xi, core]
        return send(ref, ref, u_send.at[src], z_recv.at[src], z_peer(z + 1))

    def x_copy(src):
        ref = all_s.at[src, xi, core]
        return send(ref, ref, x_send.at[src], x_recv.at[src], x_peer)

    def c_copy(src, other):
        ref = all_s.at[src, xi + other - 2 * xi * other, core]
        k = other * lines + src
        return send(ref, ref, c_send.at[k], c_recv.at[k], core_peer)

    def below(act):
        def step(d):
            @pl.when(z >= d)
            def _():
                act(d)
        return step

    d_copies = [send(d_out.at[which], d_in.at[k], d_send.at[k], d_recv.at[k], peer)
                for k, (which, peer) in enumerate(((0, x_peer), (1, xc_peer), (1, core_peer)))]
    for c in d_copies:
        c.start()
    loop(1, lines, lambda d: below(lambda e: down_copy(e).start())(lines - d))

    @pl.when(not_top)
    def _():
        up_copy(z).start()

    x_copy(z).start()
    c_copy(z, 0).start()
    load_g.wait()
    g_copy = send(g_v.at[o], g_v.at[o], y_send.at[0], y_recv.at[0], y_peer)
    p_copy = send(p_hbm.at[1 - o], p_v.at[o], y_send.at[1], y_recv.at[1], y_peer)
    g_copy.start()
    p_copy.start()

    col0 = blocks_ref[me] * cols

    def product(zz, xx):
        width = 2 * lanes
        start = pl.multiple_of((zz * 2 + xx) * width, width)
        time = (lax.broadcasted_iota(jnp.int32, (1, width), 1) + start) // orb
        one, zero = jnp.float32(1), jnp.float32(0)
        left = []
        for t in range(cols):
            keep = jnp.where((time >= col0 + t) & (time <= front_ref[o]), one, zero)
            keep = keep.astype(jnp.bfloat16)
            left += [g_v[h, t, :, pl.ds(start, width)] * keep for h in range(2)]
        right = jnp.concatenate([all_s[zz, xx, 0], all_s[zz, xx, 1]], axis=1)
        acc[...] += lax.dot_general(jnp.concatenate(left, axis=0), right, (((1,), (1,)), ((), ())),
                                    preferred_element_type=jnp.float32)

    def relay(j):
        src = source(j)
        up_copy(src).wait_recv()

        @pl.when((j <= z) & not_top)
        def _():
            up_copy(src).start()

        x_copy(src).start()
        c_copy(src, 0).start()

    def relay_x(j):
        src = source(j)
        x_copy(src).wait_recv()
        c_copy(src, 1).start()

    def near(j):
        src = source(j)
        c_copy(src, 0).wait_recv()
        product(src, xi)

    def far(j):
        src = source(j)
        c_copy(src, 1).wait_recv()
        product(src, 1 - xi)

    def dz_copy(d):
        return send(d_z.at[z], d_z.at[z], dz_send.at[d], dz_recv.at[z], z_peer(z - d))

    def dz_got(src):
        return send(d_z.at[src], d_z.at[src], dz_send.at[0], dz_recv.at[src], x_peer)

    dz_up = send(d_up, d_z.at[z], du_send, dz_recv.at[z], z_peer(z + 1))

    relay_x(0)
    for c in d_copies:
        c.wait()
    here = (d_out[0] + d_in[0]) + (d_in[1] + d_in[2])
    d_z[z] = here
    d_up[...] = here
    loop(1, lines, lambda d: below(lambda e: dz_copy(e).start())(lines - d))
    relay(1)

    @pl.when(z > 0)
    def _():
        dz_got(z - 1).wait_recv()
        d_up[...] = here + d_z[z - 1]

    @pl.when(not_top)
    def _():
        dz_up.start()

    loop(2, lines, relay)
    loop(1, lines - 1, relay_x)
    g_copy.wait_recv()
    near(0)
    near(1)
    relay_x(lines - 1)
    d_all[core] = d_up[...]

    def gather_above(src):
        @pl.when(src > z)
        def _():
            dz_got(src).wait_recv()
            d_all[core] = d_all[core] + d_z[src]

    loop(1, lines, gather_above)
    d_last = send(d_all.at[core], d_all.at[core], d_send.at[3], d_recv.at[3], core_peer)
    d_last.start()
    loop(2, lines, near)
    loop(0, lines, far)

    load_p.wait()
    p_copy.wait()
    prev = jnp.concatenate([p_v[h, t] for t in range(cols) for h in range(2)], axis=0)
    combined = acc[...] + prev
    d_last.wait()
    weight = jnp.concatenate([d_all[c][:, k * orb:(k + 1) * orb]
                              for c in range(2) for k in range(2)], axis=0)
    contract = (((1,), (1,)), ((), ()))
    high = dict(precision=lax.Precision.HIGHEST, preferred_element_type=jnp.float32)
    flipped = lax.dot_general(weight, combined, contract, **high)
    g_new = lax.dot_general(combined, weight, contract, **high)
    t_copies = []
    for t in range(cols):
        g_t = g_new[t * orb:(t + 1) * orb]
        s_t = COUPLING * g_t * g_t * flipped[:, t * orb:(t + 1) * orb]
        done = jnp.concatenate([g_t, s_t], axis=1)
        packed[t] = jnp.where(o == 0, done[half:], done[:half])
        c = send(packed.at[t], out.at[o, t], y_send.at[2 + t], y_recv.at[2 + t], y_peer)
        c.start()
        t_copies.append(c)
        out[o, t] = jnp.where(o == 0, done[:half], done[half:])

    g_copy.wait_send()
    def wait_above(src):
        @pl.when((src <= z) & not_top)
        def _():
            up_copy(src).wait_send()

    loop(0, lines, wait_above)
    loop(1, lines, below(lambda d: down_copy(d).wait_send()))
    loop(1, lines, below(lambda d: dz_copy(d).wait_send()))

    @pl.when(not_top)
    def _():
        dz_up.wait_send()

    loop(0, lines, lambda d: x_copy(d).wait_send())
    loop(0, lines, lambda d: c_copy(d, 0).wait_send())
    loop(0, lines, lambda d: c_copy(d, 1).wait_send())
    for c in t_copies:
        c.wait()


def body(lines, g_hist, sigma_hist, diag_inv, previous, block_of_slot, front_pos):
    cols, half, depth = g_hist.shape
    orb, lanes = sigma_hist.shape[1], sigma_hist.shape[2]
    smem = pl.BlockSpec(memory_space=pltpu.SMEM)
    hbm = pl.BlockSpec(memory_space=pl.ANY)
    dma = pltpu.SemaphoreType.DMA
    f32 = jnp.float32
    part = (orb // 4, 2 * orb)
    flops = 2 * cols * orb * depth * orb
    out = pl.pallas_call(
        functools.partial(kernel, lines),
        out_shape=pltpu.VMEM((2, cols, half, 2 * orb), f32),
        in_specs=[smem, smem, hbm, hbm, hbm, hbm],
        out_specs=pl.BlockSpec(memory_space=pltpu.VMEM),
        scratch_shapes=[
            pltpu.VMEM((2,) + g_hist.shape, g_hist.dtype),
            pltpu.VMEM((lines, 2, 2, orb, lanes), sigma_hist.dtype),
            pltpu.VMEM(diag_inv.shape, f32),
            pltpu.VMEM((2,) + previous.shape[1:], f32),
            pltpu.VMEM((cols * orb, orb), f32),
            pltpu.VMEM((2,) + part, f32),
            pltpu.VMEM((3,) + part, f32),
            pltpu.VMEM((lines,) + part, f32),
            pltpu.VMEM(part, f32),
            pltpu.VMEM((2,) + part, f32),
            pltpu.VMEM((cols, half, 2 * orb), f32),
            dma((4,)),
            dma((lines,)), dma((lines,)), dma((lines,)),
            dma((lines,)), dma((lines,)),
            dma((2 * lines,)), dma((2 * lines,)),
            dma((4,)), dma((4,)),
            dma((lines,)), dma((lines,)), dma(()),
            dma((2 + cols,)), dma((2 + cols,)),
        ],
        compiler_params=pltpu.CompilerParams(collective_id=0, has_side_effects=True),
        cost_estimate=pl.CostEstimate(flops=flops, bytes_accessed=2 * g_hist.size, transcendentals=0),
    )(block_of_slot, front_pos, g_hist, sigma_hist, diag_inv, previous)
    return out[..., :orb], out[..., orb:]


def solution(mesh):
    lines = mesh.shape["hist"] // 4
    in_specs = (
        P("hist", "orb", None),
        P(None, None, "hist"),
        P("hist", None, None),
        P(None, "hist", "orb", None),
        P(),
        P(),
    )
    out_specs = (P(None, "hist", "orb", None), P(None, "hist", "orb", None))
    return jax.shard_map(functools.partial(body, lines), mesh=mesh, in_specs=in_specs,
                         out_specs=out_specs, check_vma=False)
```
